32 devices in a mesh: group: 4 (over z), tensor: 8 (over y, x, core).
Axes of the slice: x: 2, y: 2, z: 4, core: 2. Of those that a mesh axis runs over, the one named last changes fastest.
Arguments:
- key_value_cache: bfloat16 [256, 1024, 256], P(('group', 'tensor')), may hold values from -8 to 8
- queries: bfloat16 [32, 48, 128], P('group'), may hold values from -200 to 200
- fresh_key_value: bfloat16 [32, 8, 256], P('group'), may hold values from -6 to 6
- lengths: int32 [32], P('group'), may hold values from 2 to 1023
- residual: bfloat16 [32, 6144], P('group'), may hold values from -100 to 100
- norm_gain: float32 [6144], replicated, may hold values from 0.1 to 1.9
- router_weight: bfloat16 [6144, 8], replicated, may hold values from -0.078125 to 0.078125
- routing: int32 [32, 2], P('group'), may hold values from 0 to 7, all different within a row
- expert_gate: bfloat16 [8, 6144, 8192], P(None, 'group', 'tensor'), may hold values from -0.078125 to 0.078125
- expert_up: bfloat16 [8, 6144, 8192], P(None, 'group', 'tensor'), may hold values from -0.078125 to 0.078125
Outputs:
- updated: bfloat16 [32, 6144], P('group')
- expert_hidden: bfloat16 [32, 2, 8192], P('group', None, 'tensor')
- new_cache: bfloat16 [32, 8, 1024, 256], P('group', None, 'tensor')
The draws below stay inside these ranges and needn't reach their ends.
Inputs may be any that keep to these rules, and one draw needn't show every extreme that they name: Slot lengths[s] of sequence s receives its new token. `routing`: A token's two experts differ.
All inputs are finite; a program needn't handle non-finite values.
Results may differ from the reference program's by a relative error of at most 0.028.
Values may be sent and summed in bfloat16 or wider, within the bound.
No kernel may reach another device: no remote copies, remote signals or barrier semaphores. Data moves between devices by JAX's collectives and lax.ppermute only.
A program may use at most 128 MiB of HBM per device.

```python
import math
import jax
import jax.numpy as jnp
from jax import lax

D = 6144
QUERY_HEADS = 48
KEY_VALUE_HEADS = 8
HEAD_DIM = 128
EXPERTS = 8
TOPK = 2
FF_WIN = 8192
CONTEXT_SLOTS = 1024
SEQUENCE_TOTAL = 32


def starting_cache(key):
    cache_random_key = jax.random.fold_in(key, 7)
    return jnp.clip(jax.random.normal(cache_random_key, (SEQUENCE_TOTAL * KEY_VALUE_HEADS, CONTEXT_SLOTS, 2 * HEAD_DIM), jnp.float32), -6.0, 6.0)


def draw_key_value_cache(key, part):
    cache_layout_grid = starting_cache(key)
    return cache_layout_grid.astype(jnp.bfloat16)


def draw_queries(key, part):
    query_group_width = QUERY_HEADS // KEY_VALUE_HEADS
    query_vectors = jnp.clip(jax.random.normal(jax.random.fold_in(key, 21), (SEQUENCE_TOTAL, KEY_VALUE_HEADS, query_group_width, HEAD_DIM), jnp.float32), -4.0, 4.0)
    return query_vectors.reshape(SEQUENCE_TOTAL, QUERY_HEADS, HEAD_DIM).astype(jnp.bfloat16)


def draw_residual(key, part):
    base_key = jax.random.fold_in(key, 31)
    row_key = jax.random.fold_in(key, 32)
    column_key = jax.random.fold_in(key, 33)
    values = jnp.clip(jax.random.normal(base_key, (SEQUENCE_TOTAL, D), jnp.float32), -4.0, 4.0)
    row_scale = jnp.exp(jax.random.uniform(row_key, (SEQUENCE_TOTAL, 1), jnp.float32, jnp.log(0.4), jnp.log(4.0)))
    column_scale = jnp.exp(jax.random.uniform(column_key, (1, D), jnp.float32, jnp.log(0.4), jnp.log(4.0)))
    return (values * row_scale * column_scale).astype(jnp.bfloat16)


def touch_ends(values, rng, least, high):
    dims = values.shape
    spot = [jax.random.randint(jax.random.fold_in(rng, axis), (), 0, dims[axis]) for axis in range(len(dims))]
    values = values.at[tuple(spot)].set(least)
    longest = dims.index(max(dims))
    spot[longest] = (spot[longest] + 1) % dims[longest]
    return values.at[tuple(spot)].set(high)


def shard_levels(rng, shape, pieces, smallest, high):
    level, own = 1.0, jax.random.fold_in(rng, 6)
    for position, shards_of in pieces:
        heights = jnp.exp(jax.random.uniform(jax.random.fold_in(own, position), (shards_of,), jnp.float32, smallest / len(pieces), high / len(pieces)))
        level = level * jnp.repeat(heights, shape[position] // shards_of).reshape([-1 if axis == position else 1 for axis in range(len(shape))])
    return level


def picks_of(key, rows, amount, top, lift):
    sequence = jax.random.permutation(jax.random.fold_in(key, 1), amount)
    boost = sequence
    for power in range(3):
        boost = boost * boost // amount
    boost = boost * lift // amount
    tickets = jax.random.randint(jax.random.fold_in(key, 2), (rows, amount), 0, 4096) + boost
    holders = jax.random.permutation(jax.random.fold_in(key, 3), rows)[jnp.arange(amount) % rows]
    tickets = jnp.where(jnp.arange(rows)[:, None] == holders[None, :], 1 << 14, tickets)
    merit = tickets * amount + jnp.arange(amount)
    return lax.top_k(merit.astype(jnp.int32), top)[1].astype(jnp.int32)


def scatter_about(key, extent, scale, limit, shards=(), kind=jnp.bfloat16):
    loudness = shard_levels(key, extent, shards, -0.22, 0.18) if shards else 1.0
    values = jax.random.normal(key, extent, jnp.float32) * scale * loudness
    return jnp.minimum(jnp.maximum(values, -limit), limit).astype(kind)


def setup_inputs(seed: int = 0) -> dict:
    key_of = jax.random.split(jax.random.key(seed), 11)
    return {
        "key_value_cache": draw_key_value_cache(jax.random.fold_in(key_of[10], 71), 0),
        "queries": draw_queries(jax.random.fold_in(key_of[10], 71), 0),
        "fresh_key_value": scatter_about(key_of[2], (SEQUENCE_TOTAL, KEY_VALUE_HEADS, 2 * HEAD_DIM), 1.0, 6.0, ((0, 4),)),
        "lengths": touch_ends(jax.random.randint(key_of[3], (SEQUENCE_TOTAL,), 2, CONTEXT_SLOTS), jax.random.fold_in(key_of[3], 1), 2, CONTEXT_SLOTS - 1).astype(jnp.int32),
        "residual": draw_residual(jax.random.fold_in(key_of[10], 71), 0),
        "norm_gain": jnp.clip(1.0 + 0.18 * jax.random.normal(key_of[5], (D,), jnp.float32), 0.1, 1.9),
        "router_weight": scatter_about(key_of[6], (D, EXPERTS), D ** -0.5, 0.078125),
        "routing": picks_of(key_of[7], SEQUENCE_TOTAL, EXPERTS, TOPK, 2048),
        "expert_gate": scatter_about(key_of[8], (EXPERTS, D, FF_WIN), D ** -0.5, 0.078125, ((1, 4), (2, 8))),
        "expert_up": scatter_about(key_of[9], (EXPERTS, D, FF_WIN), D ** -0.5, 0.078125, ((1, 4), (2, 8))),
    }


def reference(key_value_cache, queries, fresh_key_value, lengths, residual, norm_gain, router_weight, routing, expert_gate, expert_up):
    query_group_width = QUERY_HEADS // KEY_VALUE_HEADS
    cache_layout_grid = key_value_cache.reshape(SEQUENCE_TOTAL, KEY_VALUE_HEADS, CONTEXT_SLOTS, 2 * HEAD_DIM)
    key_rows = cache_layout_grid[..., :HEAD_DIM].astype(jnp.float32)
    value_rows = cache_layout_grid[..., HEAD_DIM:].astype(jnp.float32)
    query_vectors = queries.reshape(SEQUENCE_TOTAL, KEY_VALUE_HEADS, query_group_width, HEAD_DIM).astype(jnp.float32)
    score_scale = 1.0 / math.sqrt(HEAD_DIM)
    scores = jnp.einsum('sngd,sntd->sngt', query_vectors, key_rows, precision=lax.Precision.HIGHEST) * score_scale
    own_key = fresh_key_value[..., :HEAD_DIM].astype(jnp.float32)
    own_value = fresh_key_value[..., HEAD_DIM:].astype(jnp.float32)
    own_score = jnp.einsum('sngd,snd->sng', query_vectors, own_key, precision=lax.Precision.HIGHEST) * score_scale
    visible = jnp.arange(CONTEXT_SLOTS, dtype=jnp.int32)[None, None, None, :] < lengths[:, None, None, None]
    peak = jnp.maximum(lax.optimization_barrier(jnp.max(jnp.where(visible, scores, -jnp.inf), -1)), own_score)
    attention_weights = jnp.where(visible, jnp.exp(scores - peak[..., None]), 0.0)
    own_weight = jnp.exp(own_score - peak)
    denominator = lax.optimization_barrier(jnp.sum(attention_weights, -1)) + own_weight
    rounded = lax.optimization_barrier(attention_weights.astype(jnp.bfloat16)).astype(jnp.float32)
    own_rounded = lax.optimization_barrier(own_weight.astype(jnp.bfloat16)).astype(jnp.float32)
    weighted = jnp.einsum('sngt,sntd->sngd', rounded, value_rows, precision=lax.Precision.HIGHEST)
    weighted = weighted + own_rounded[..., None] * own_value[:, :, None, :]
    attention = (weighted / denominator[..., None]).reshape(SEQUENCE_TOTAL, D)
    updated = (residual.astype(jnp.float32) + attention).astype(jnp.bfloat16)
    stream = updated.astype(jnp.float32)
    normed = (stream * lax.rsqrt(lax.optimization_barrier(jnp.mean(stream * stream, -1, keepdims=True)) + 1e-05) * norm_gain).astype(jnp.bfloat16)
    logits = jnp.dot(normed, router_weight, preferred_element_type=jnp.float32)
    chosen_mask = routing[:, :, None] == jnp.arange(EXPERTS, dtype=jnp.int32)[None, None, :]
    chosen_logits = lax.optimization_barrier(jnp.sum(jnp.where(chosen_mask, logits[:, None, :], 0.0), -1))
    gate_weights = jax.nn.sigmoid(chosen_logits - chosen_logits[:, ::-1])

    def expert_pass(weight_pair):
        gate_part = jnp.dot(normed, weight_pair[0], preferred_element_type=jnp.float32)
        up_part = jnp.dot(normed, weight_pair[1], preferred_element_type=jnp.float32)
        return jnp.stack((gate_part, up_part), 1)
    every_expert = lax.map(expert_pass, (expert_gate, expert_up))
    every_expert = jnp.transpose(every_expert, (1, 0, 2, 3))
    picked = lax.optimization_barrier(jnp.sum(jnp.where(chosen_mask[:, :, :, None, None], every_expert[:, None], 0.0), 2))
    expert_hidden = (gate_weights[:, :, None] * jax.nn.silu(picked[:, :, 0]) * picked[:, :, 1]).astype(jnp.bfloat16)
    new_slot = jnp.arange(CONTEXT_SLOTS, dtype=jnp.int32)[None, None, :, None] == lengths[:, None, None, None]
    new_cache = jnp.where(new_slot, fresh_key_value[:, :, None, :], cache_layout_grid)
    return (updated, expert_hidden, new_cache)
```

```python
import math

import jax
import jax.numpy as jnp
from jax import lax
from jax.experimental import pallas as pl
from jax.experimental.pallas import tpu as pltpu
from jax.sharding import PartitionSpec as P

F32 = jnp.float32
BF16 = jnp.bfloat16


def attend(lengths, place, key_value_cache, queries, fresh, ranks):
    pairs, slots, width = key_value_cache.shape
    kv_heads = fresh.shape[1]
    seq_local, q_heads, head_size = queries.shape
    heads = q_heads // kv_heads
    span = slots // ranks
    score_scale = 1.0 / math.sqrt(head_size)
    step = 4 if pairs % 4 == 0 else pairs
    steps = pairs // step
    query_rows = queries.reshape(seq_local * q_heads, head_size)
    own_rows = fresh.reshape(seq_local * kv_heads, width)
    aligned = pairs % 8 == 0
    if not aligned:
        query_rows = lax.dynamic_slice_in_dim(
            query_rows, place[0] * pairs * heads, pairs * heads, 0
        )
        own_rows = lax.dynamic_slice_in_dim(own_rows, place[0] * pairs, pairs, 0)

    def kernel(length_ref, place_ref, cache_ref, query_ref, own_ref, *refs):
        send_refs, result_ref, row_ref = refs[:ranks], refs[ranks], refs[ranks + 1]
        place = place_ref[0]

        def work(base):
            for i in range(step):
                pair = base + i
                length = length_ref[(place * pairs + pair) // kv_heads]
                slot = lax.broadcasted_iota(jnp.int32, (slots, 1), 0)
                row_ref[i] = jnp.where(slot == length, own_ref[pair : pair + 1, :], cache_ref[i])
                for d in range(ranks):
                    begin = pl.multiple_of((place ^ d) * span, span)
                    send_refs[d][i] = row_ref[i, pl.ds(begin, span), :]
                query = query_ref[pair * heads : (pair + 1) * heads, :]
                scores = (
                    lax.dot_general(
                        query,
                        row_ref[i, :, :head_size],
                        (((1,), (1,)), ((), ())),
                        preferred_element_type=F32,
                    )
                    * score_scale
                )
                visible = lax.broadcasted_iota(jnp.int32, (heads, slots), 1) <= length
                scores = jnp.where(visible, scores, -1e30)
                peak = jnp.max(scores, -1, keepdims=True)
                weights = jnp.where(visible, jnp.exp(scores - peak), 0.0)
                denominator = jnp.sum(weights, -1, keepdims=True)
                weighted = jnp.dot(
                    weights.astype(BF16), row_ref[i, :, head_size:], preferred_element_type=F32
                )
                result_ref[pair * heads : (pair + 1) * heads, :] = weighted / denominator

        for n in range(steps):
            pl.when(pl.program_id(0) == n)(lambda n=n: work(n * step))

    mine = (lambda i, _, place: (place[0], 0)) if aligned else (lambda i, *_: (0, 0))
    kept = lambda i, _, place: (place[0] * steps + i, 0, 0)
    return pl.pallas_call(
        kernel,
        grid_spec=pltpu.PrefetchScalarGridSpec(
            num_scalar_prefetch=2,
            grid=(steps,),
            in_specs=[
                pl.BlockSpec((step, slots, width), lambda i, *_: (i, 0, 0)),
                pl.BlockSpec((pairs * heads, head_size), mine),
                pl.BlockSpec((pairs, width), mine),
            ],
            out_specs=[pl.BlockSpec((step, span, width), kept)]
            + [pl.BlockSpec((step, span, width), lambda i, *_: (i, 0, 0))] * (ranks - 1)
            + [pl.BlockSpec((pairs * heads, head_size), lambda i, *_: (0, 0))],
            scratch_shapes=[pltpu.VMEM((step, slots, width), BF16)],
        ),
        out_shape=[jax.ShapeDtypeStruct((ranks * pairs, span, width), BF16)]
        + [jax.ShapeDtypeStruct((pairs, span, width), BF16)] * (ranks - 1)
        + [jax.ShapeDtypeStruct((pairs * heads, head_size), F32)],
        name="attend",
    )(lengths, place, key_value_cache, query_rows, own_rows)


def normalize(gathered, residual, gain, router, routing, groups):
    local, model = residual.shape
    lanes = gathered.shape[1]
    chunks = model // lanes
    count = router.shape[0]
    picks = routing.shape[1]
    share = chunks // groups

    def kernel(gathered_ref, residual_ref, gain_ref, router_ref, routing_ref,
               updated_ref, message_ref, weight_ref, normed_ref):
        square = jnp.zeros((local, lanes), F32)
        for c in range(chunks):
            part = slice(c * lanes, (c + 1) * lanes)
            value = residual_ref[:, part].astype(F32) + gathered_ref[pl.ds(c, local, stride=chunks), :]
            value = value.astype(BF16)
            updated_ref[:, part] = value
            value = value.astype(F32)
            square += value * value
        factor = lax.rsqrt(jnp.sum(square, -1, keepdims=True) / model + 1e-05)
        for c in range(chunks):
            part = slice(c * lanes, (c + 1) * lanes)
            value = (updated_ref[:, part].astype(F32) * factor * gain_ref[:, part]).astype(BF16)
            normed_ref[:, part] = value
            message_ref[c // share, :, c % share * lanes : (c % share + 1) * lanes] = value
        choice = routing_ref[...]
        lane = lax.broadcasted_iota(jnp.int32, (local, lanes), 1)
        packed = jnp.zeros((local, lanes), F32)
        for k in range(picks):
            packed = jnp.where(lane == k, choice[:, k : k + 1].astype(F32), packed)
        for g in range(groups):
            message_ref[g, :, share * lanes :] = packed.astype(BF16)
        logits = lax.dot_general(
            normed_ref[...],
            router_ref[...],
            (((1,), (1,)), ((), ())),
            preferred_element_type=F32,
        )
        ids = lax.broadcasted_iota(jnp.int32, (local, count), 1)
        chosen = [
            jnp.sum(jnp.where(choice[:, k : k + 1] == ids, logits, 0.0), -1, keepdims=True)
            for k in range(picks)
        ]
        for k in range(picks):
            weight_ref[k] = jnp.broadcast_to(
                jax.nn.sigmoid(chosen[k] - chosen[picks - 1 - k]), (local, lanes)
            )

    return pl.pallas_call(
        kernel,
        out_shape=[
            jax.ShapeDtypeStruct((local, model), BF16),
            jax.ShapeDtypeStruct((groups, local, (share + 1) * lanes), BF16),
            jax.ShapeDtypeStruct((picks, local, lanes), F32),
        ],
        scratch_shapes=[pltpu.VMEM((local, model), BF16)],
        name="normalize",
    )(gathered, residual, gain, router, routing)


def experts(message, gate, up, groups, picks):
    tokens = message.shape[0]
    count, columns, hidden = gate.shape
    local = tokens // groups
    block = hidden // 2 if hidden % 256 == 0 else hidden

    def kernel(message_ref, gate_ref, up_ref, part_ref, total_ref):
        expert = pl.program_id(1)
        x = message_ref[:, :columns]
        sums = [jnp.dot(x, ref[0], preferred_element_type=F32) for ref in (gate_ref, up_ref)]
        routing = message_ref[:, columns:].astype(F32)
        for k in range(picks):
            picked = routing[:, k : k + 1] == expert.astype(F32)
            for n in range(2):
                total_ref[2 * k + n] = jnp.where(picked, sums[n], total_ref[2 * k + n])

        @pl.when(expert == count - 1)
        def _():
            for j in range(2 * picks):
                for g in range(groups):
                    part_ref[g, j] = total_ref[j, g * local : (g + 1) * local, :].astype(BF16)

    weights = pl.BlockSpec((1, columns, block), lambda h, e: (e, 0, h))
    return pl.pallas_call(
        kernel,
        grid=(hidden // block, count),
        in_specs=[pl.BlockSpec(message.shape, lambda h, e: (0, 0)), weights, weights],
        out_specs=pl.BlockSpec((groups, 2 * picks, local, block), lambda h, e: (0, 0, 0, h)),
        out_shape=jax.ShapeDtypeStruct((groups, 2 * picks, local, hidden), BF16),
        scratch_shapes=[pltpu.VMEM((2 * picks, tokens, block), F32)],
        name="experts",
    )(message, gate, up)


def combine(arrived, weight):
    groups, sums, local, hidden = arrived.shape
    picks = sums // 2

    def kernel(arrived_ref, weight_ref, out_ref):
        for k in range(picks):
            gate, up = (
                sum(arrived_ref[g, 2 * k + n].astype(F32) for g in range(groups))
                for n in range(2)
            )
            factor = weight_ref[k][:, :1]
            silu = gate / (1.0 + jnp.exp(-gate))
            out_ref[:, k, :] = (factor * silu * up).astype(BF16)

    return pl.pallas_call(
        kernel,
        out_shape=jax.ShapeDtypeStruct((local, picks, hidden), BF16),
        name="combine",
    )(arrived, weight)


def body(
    key_value_cache,
    queries,
    fresh_key_value,
    lengths,
    residual,
    norm_gain,
    router_weight,
    routing,
    expert_gate,
    expert_up,
):
    tensor_rank = lax.axis_index("tensor")
    groups, ranks = lax.axis_size("group"), lax.axis_size("tensor")
    seq_local = queries.shape[0]
    kv_heads = fresh_key_value.shape[1]
    pairs, slots, width = key_value_cache.shape
    place = tensor_rank[None].astype(jnp.int32)

    rows, *send, result = attend(lengths, place, key_value_cache, queries, fresh_key_value, ranks)
    with jax.named_scope("gather"):
        gathered = lax.all_gather(result, "tensor", axis=0, tiled=True)
    gathered, send = lax.optimization_barrier((gathered, send))
    updated, message, weight = normalize(
        gathered, residual, norm_gain[None], router_weight.T, routing, groups
    )
    with jax.named_scope("columns"):
        message = lax.all_to_all(message, "group", split_axis=0, concat_axis=0, tiled=True)
    part = experts(
        message.reshape(groups * seq_local, -1), expert_gate, expert_up, groups, routing.shape[1]
    )
    with jax.named_scope("partials"):
        arrived = lax.all_to_all(part, "group", split_axis=0, concat_axis=0, tiled=True)
    expert_hidden = combine(arrived, weight)

    moved = []
    for i in range(1, ranks):
        with jax.named_scope(f"move{i}"):
            moved.append(lax.ppermute(send[i - 1], "tensor", [(r, r ^ i) for r in range(ranks)]))
    for i in range(1, ranks):
        rows = lax.dynamic_update_slice_in_dim(rows, moved[i - 1], (tensor_rank ^ i) * pairs, 0)
    new_cache = rows.reshape(seq_local, kv_heads, slots // ranks, width)
    return (updated, expert_hidden, new_cache)


def solution(mesh):
    in_specs = (
        P(("group", "tensor"), None, None),
        P("group", None, None),
        P("group", None, None),
        P("group"),
        P("group", None),
        P(),
        P(),
        P("group", None),
        P(None, "group", "tensor"),
        P(None, "group", "tensor"),
    )
    out_specs = (P("group", None), P("group", None, "tensor"), P("group", None, "tensor", None))
    return jax.shard_map(body, mesh=mesh, in_specs=in_specs, out_specs=out_specs, check_vma=False)
```
